256 devices in a mesh: gx: 16 (over x, z_lo, core), gy: 4 (over y), gz: 4 (over z_hi).
Axes of the slice: x: 4, y: 4, z: 8 (z_hi: 4, z_lo: 2; z = z_hi * 2 + z_lo), core: 2. Of those that a mesh axis runs over, the one named last changes fastest.
Arguments:
- right_side: float32 [4, 5, 16, 32, 512], P(None, None, 'gx', 'gy', 'gz'), may hold values from -6 to 6
- jacobian: bfloat16 [27, 5, 5, 16, 32, 512], P(None, None, None, 'gx', 'gy', 'gz'), may hold values from -0.14 to 12.14, as said below
Outputs:
- solution: float32 [4, 5, 16, 32, 512], P(None, None, 'gx', 'gy', 'gz')
- residual: float32 [4, 5, 16, 32, 512], P(None, None, 'gx', 'gy', 'gz')
The draws below stay inside these ranges and needn't reach their ends.
Inputs may be any that keep to these rules, and one draw needn't show every extreme that they name: `jacobian`: blocks of offsets other than 13 and the off-diagonal entries of block 13 lie within -0.14 to 0.14; the diagonal entries of block 13 exceed 5.8 in every cell.
All inputs are finite; a program needn't handle non-finite values.
Results may differ from the reference program's by a relative error of at most 0.0003.
Values sent between devices are 32-bit elements.
A program may use at most 64 MiB of HBM per device.

```python
import jax
import jax.numpy as jnp
from jax import lax

COMP = 5
RHS = 4
STENCIL = 27
ITERS = 3
NX = 16
NY = 32
NZ = 512


def draw_jacobian(key, part):
    first_key, second_key = jax.random.split(jax.random.fold_in(key, 17))
    full_shape = (STENCIL, COMP, COMP, NX, NY, NZ)
    diag_shape = (COMP, NX, NY, NZ)
    entries = jax.random.uniform(first_key, full_shape, jnp.float32, -0.14, 0.14)
    diagonal = jax.random.uniform(second_key, diag_shape, jnp.float32, 6.0, 12.0)
    identity = jnp.eye(COMP, dtype=jnp.float32)[:, :, None, None, None]
    center = entries[13] + identity * diagonal[:, None]
    entries = entries.at[13].set(center)
    return entries.astype(jnp.bfloat16)


def levels(rng, extent, shards, least, high):
    level = 1.0
    for axis_at, blocks in shards:
        heights = jax.random.uniform(jax.random.fold_in(jax.random.fold_in(rng, 6), axis_at), (blocks,), jnp.float32, least / len(shards), high / len(shards))
        level = level * jnp.repeat(jnp.exp(heights), extent[axis_at] // blocks).reshape((-1,) + (1,) * (len(extent) - 1 - axis_at))
    return level


def noise(rng, extent, deviation, bound, shards=(), kind=jnp.bfloat16):
    array = jax.random.normal(rng, extent, jnp.float32) * deviation
    if len(shards) > 0:
        array = levels(rng, extent, shards, -0.22, 0.18) * array
    return jnp.clip(array, min=-bound, max=bound).astype(kind)


def setup_inputs(seed: int = 0) -> dict:
    streams_of = jax.random.split(jax.random.key(seed), 3)
    return {
        "right_side": noise(streams_of[0], (RHS, COMP, NX, NY, NZ), 1.0, 6.0, ((2, 16), (3, 4), (4, 4)), jnp.float32),
        "jacobian": draw_jacobian(jax.random.fold_in(streams_of[2], 71), 0),
    }


def dot_high(left, right):
    return jnp.dot(left.astype(jnp.float32), right.astype(jnp.float32), precision=lax.Precision.HIGHEST, preferred_element_type=jnp.float32)

def lower_solve(factor, target):
    solved = []
    for row_pos in range(factor.shape[0]):
        accum = target[row_pos]
        for prior in range(row_pos):
            accum = accum - factor[row_pos, prior] * solved[prior]
        solved.append(accum / factor[row_pos, row_pos])
    return jnp.stack(solved)

def upper_solve(factor, target):
    size_all = factor.shape[0]
    solved = [None] * size_all
    for row_pos in range(size_all - 1, -1, -1):
        accum = target[row_pos]
        for later in range(row_pos + 1, size_all):
            accum = accum - factor[later, row_pos] * solved[later]
        solved[row_pos] = accum / factor[row_pos, row_pos]
    return jnp.stack(solved)

def extend(field):
    padded = jnp.pad(field, ((0, 0), (0, 0), (1, 1), (1, 1), (0, 0)), mode='wrap')
    return jnp.pad(padded, ((0, 0), (0, 0), (0, 0), (0, 0), (1, 1)))

def apply_operator(jacobian, padded):
    extent_x = padded.shape[2] - 2
    extent_y = padded.shape[3] - 2
    extent_z = padded.shape[4] - 2
    total = jnp.zeros((padded.shape[0], padded.shape[1], extent_x, extent_y, extent_z), jnp.float32)
    for stencil_pos in range(27):
        start_x = stencil_pos // 9
        start_y = stencil_pos // 3 % 3
        start_z = stencil_pos % 3
        piece = padded[:, :, start_x:start_x + extent_x, start_y:start_y + extent_y, start_z:start_z + extent_z]
        block = jacobian[stencil_pos].astype(jnp.float32)
        for source_comp in range(block.shape[1]):
            total = total + block[None, :, source_comp] * piece[:, source_comp][:, None]
    return total

def reference(right_side, jacobian):
    field_shape = right_side.shape
    rhs_count = field_shape[0]
    flat_rhs = right_side.reshape(rhs_count, -1)
    start_factor = jnp.linalg.cholesky(dot_high(flat_rhs, flat_rhs.T))
    basis = [lower_solve(start_factor, flat_rhs)]
    hessen_rows = []
    for iteration in range(ITERS):
        workspace = apply_operator(jacobian, extend(basis[-1].reshape(field_shape))).reshape(rhs_count, -1)
        stacked = jnp.concatenate(basis, axis=0)
        coefficients = dot_high(stacked, workspace.T)
        workspace = workspace - dot_high(coefficients.T, stacked)
        factor = jnp.linalg.cholesky(dot_high(workspace, workspace.T))
        basis.append(lower_solve(factor, workspace))
        filler = jnp.zeros((rhs_count, rhs_count * (ITERS - iteration - 1)), jnp.float32)
        hessen_rows.append(jnp.concatenate([coefficients.T, factor, filler], axis=1))
    hessen = jnp.concatenate(hessen_rows, axis=0)
    target = jnp.concatenate([start_factor, jnp.zeros((rhs_count, rhs_count * ITERS), jnp.float32)], axis=1)
    normal_factor = jnp.linalg.cholesky(dot_high(hessen, hessen.T))
    middle = lower_solve(normal_factor, dot_high(hessen, target.T))
    weights = upper_solve(normal_factor, middle)
    solution = dot_high(weights.T, jnp.concatenate(basis[:-1], axis=0))
    solution_field = solution.reshape(field_shape)
    residual = right_side - apply_operator(jacobian, extend(solution_field))
    return (solution_field, residual)
```

```python
import jax
import jax.numpy as jnp
from jax import lax
from jax.experimental import pallas as pl
from jax.experimental.pallas import tpu as pltpu
from jax.sharding import PartitionSpec as P

MESH = pl.DeviceIdType.MESH
SHIFT = 9.0
BETA1 = 3.9
BETA2 = 3.2
STEPS = 3
ROW = 8

OFFSETS = [
    (ex, ey, ez)
    for ey, ez in ((0, 0), (0, -1), (0, 1), (-1, 0), (1, 0), (-1, -1), (-1, 1), (1, -1), (1, 1))
    for ex in (-1, 1, 0)
    if (ex, ey, ez) != (0, 0, 0)
]


def side(sign):
    return (sign + 1) // 2


def make_kernel(nx, ny, nz):
    group_a = (nx // 4) * ny
    group_b = 4 * nz

    def kernel(
        rhs_ref, jac_hbm, sol_ref, res_ref,
        jac_raw, jac, basis, slab, rowbuf, colbuf, corbuf, rowsrc, colsrc, corsrc, padded,
        gramsrc, sumsrc, gather_a, gather_b,
        jac_sem, halo_send, halo_recv, a_send, a_recv, b_send, b_recv,
    ):
        ix, iy, iz = lax.axis_index("gx"), lax.axis_index("gy"), lax.axis_index("gz")

        def neighbour(offset):
            ex, ey, ez = offset
            return (
                lax.rem(ix + ex + nx, nx),
                lax.rem(iy + ey + ny, ny),
                lax.rem(iz + ez + nz, nz),
            )

        rank_a = (ix // 4) * ny + iy
        rank_b = lax.rem(ix, 4) * nz + iz

        def partner_a(offset):
            rank = lax.rem(rank_a + offset, group_a)
            return ((rank // ny) * 4 + lax.rem(ix, 4), lax.rem(rank, ny), iz)

        def partner_b(offset):
            rank = lax.rem(rank_b + offset, group_b)
            return ((ix // 4) * 4 + rank // nz, iy, lax.rem(rank, nz))

        jac_copy = pltpu.make_async_copy(jac_hbm, jac_raw, jac_sem)
        jac_copy.start()

        barrier = pltpu.get_barrier_semaphore()
        partners = [neighbour(offset) for offset in OFFSETS]
        partners += [partner_a(offset) for offset in range(1, group_a)]
        partners += [partner_b(offset) for offset in range(1, group_b)]
        for partner in partners:
            pl.semaphore_signal(barrier, inc=1, device_id=partner, device_id_type=MESH)

        lane = lax.broadcasted_iota(jnp.int32, (8, 128), 1)
        lane3 = lax.broadcasted_iota(jnp.int32, (4, 8, 128), 2)
        at_low = iz == 0
        at_high = iz == nz - 1

        def halo_copies(step):
            copies = []
            for index, offset in enumerate(OFFSETS):
                ex, ey, ez = offset
                if ey == 0 and ez == 0:
                    src, dst = basis.at[step], slab.at[step, side(-ex)]
                elif ez == 0:
                    src, dst = rowsrc.at[step, side(ey)], rowbuf.at[step, 1 - ex, side(-ey)]
                elif ey == 0:
                    src, dst = colsrc.at[step, side(ez)], colbuf.at[step, 1 - ex, side(-ez)]
                else:
                    src = corsrc.at[step, 2 * side(ey) + side(ez)]
                    dst = corbuf.at[step, 1 - ex, 2 * side(-ey) + side(-ez)]
                copies.append(
                    pltpu.make_async_remote_copy(
                        src_ref=src,
                        dst_ref=dst,
                        send_sem=halo_send.at[step, index],
                        recv_sem=halo_recv.at[step, index],
                        device_id=neighbour(offset),
                        device_id_type=MESH,
                    )
                )
            return copies

        def pack(step):
            low = jnp.zeros((8, 128), jnp.float32)
            high = jnp.zeros((8, 128), jnp.float32)
            for r in range(4):
                for b in range(5):
                    field = 5 * r + b
                    tile = basis[step, r, b]
                    low = jnp.where(lane == field, pltpu.roll(tile, field, 1) if field else tile, low)
                    high = jnp.where(lane == field, pltpu.roll(tile, field + 1, 1), high)
                    rowsrc[step, 0, field : field + 1, :] = tile[0:1, :]
                    rowsrc[step, 1, field : field + 1, :] = tile[7:8, :]
            colsrc[step, 0] = low
            colsrc[step, 1] = high
            for pos in range(2):
                edge = slice(7 * pos, 7 * pos + 1)
                corsrc[step, 2 * pos] = low[edge, :]
                corsrc[step, 2 * pos + 1] = high[edge, :]

        row_id = lax.broadcasted_iota(jnp.int32, (24, 128), 0)
        lane_row = lax.broadcasted_iota(jnp.int32, (24, 128), 1)

        def fill(step, plane, source):
            for dz in (-1, 0, 1):
                if dz != 0:
                    column = colbuf[step, plane, side(dz)]
                    outside = at_low if dz < 0 else at_high
                    column = jnp.where(outside, jnp.zeros_like(column), column)
                    edge_lane = 0 if dz < 0 else 127
                    turn = 1 if dz < 0 else 127
                for r in range(4):
                    for b in range(5):
                        tile = source[r, b]
                        if dz != 0:
                            field = 5 * r + b
                            shift = (edge_lane - field) % 128
                            moved = pltpu.roll(column, shift, 1) if shift else column
                            tile = jnp.where(lane == edge_lane, moved, pltpu.roll(tile, turn, 1))
                        padded[plane, dz + 1, r, b, ROW : ROW + 8, :] = tile
                for dy in (-1, 1):
                    rows = rowbuf[step, plane, side(dy)]
                    if dz != 0:
                        corner = corbuf[step, plane, 2 * side(dy) + side(dz)]
                        spread = jnp.broadcast_to(corner, (24, 128))
                        spread = jnp.where(row_id == lane_row, spread, 0.0)
                        corner_column = jnp.sum(spread, axis=1, keepdims=True)
                        corner_column = jnp.where(outside, jnp.zeros_like(corner_column), corner_column)
                        rows = jnp.where(lane_row == edge_lane, corner_column, pltpu.roll(rows, turn, 1))
                    target = ROW - 1 if dy < 0 else ROW + 8
                    for r in range(4):
                        for b in range(5):
                            field = 5 * r + b
                            padded[plane, dz + 1, r, b, target : target + 1, :] = rows[field : field + 1, :]

        def accumulate(plane, totals):
            def at_dz(dzi, totals):
                totals = list(totals)
                for dyi in range(3):
                    start = ROW - 1 + dyi
                    s = plane * 9 + dyi * 3 + dzi
                    for b in range(5):
                        values = padded[plane, dzi, :, b, start : start + 8, :]
                        for a in range(5):
                            totals[a] = totals[a] + jac[s * 25 + 5 * a + b][None] * values
                return tuple(totals)

            return lax.fori_loop(0, 3, at_dz, totals)

        def gram_block(block):
            gram = jnp.zeros((4, 128), jnp.float32)
            lanes = lax.broadcasted_iota(jnp.int32, (4, 128), 1)
            for n in range(4 * block + 4):
                product = basis[block, :, 0] * basis[n // 4, n % 4, 0][None]
                for b in range(1, 5):
                    product = product + basis[block, :, b] * basis[n // 4, n % 4, b][None]
                partial = jnp.sum(jnp.sum(product, axis=1), axis=1, keepdims=True)
                gram = jnp.where(lanes == 16 * block + n, partial, gram)
            return gram

        basis[0] = rhs_ref[...]
        pack(0)
        jac_copy.wait()

        def unpack(s, carry):
            rows = pl.ds(s * 25, 25)
            jac[rows] = jac_raw[rows].astype(jnp.float32)
            return carry

        lax.fori_loop(0, 27, unpack, 0)
        for a in range(5):
            jac[13 * 25 + 6 * a] = jac[13 * 25 + 6 * a] - SHIFT

        pl.semaphore_wait(barrier, len(partners))

        sent = []
        gram = jnp.zeros((4, 128), jnp.float32)
        for step in range(STEPS):
            copies = halo_copies(step)
            for copy in copies:
                copy.start()
            sent += copies
            gram = gram + gram_block(step)
            totals = tuple(jnp.zeros((4, 8, 128), jnp.float32) for _ in range(5))
            for plane in (1, 0, 2):
                for copy, offset in zip(copies, OFFSETS):
                    if 1 - offset[0] == plane:
                        copy.wait_recv()
                fill(step, plane, basis.at[step] if plane == 1 else slab.at[step, plane // 2])
                totals = accumulate(plane, totals)
            for a in range(5):
                value = totals[a]
                if step == 1:
                    value = value - BETA1 * basis[0, :, a]
                if step == 2:
                    value = value - BETA2 * basis[1, :, a]
                basis[step + 1, :, a] = value
            if step + 1 < STEPS:
                pack(step + 1)
        gram = gram + gram_block(3)

        def gather(partial, size, rank, partner, src, slots, send, recv):
            src[...] = partial
            slots[rank] = partial
            copies = []
            for offset in range(1, size):
                copies.append(
                    pltpu.make_async_remote_copy(
                        src_ref=src,
                        dst_ref=slots.at[rank],
                        send_sem=send.at[offset],
                        recv_sem=recv.at[offset],
                        device_id=partner(offset),
                        device_id_type=MESH,
                    )
                )
            for copy in copies:
                copy.start()
            for copy in copies:
                copy.wait_recv()
            parts = [slots[i] for i in range(size)]
            while len(parts) > 1:
                parts = [parts[i] + parts[i + 1] if i + 1 < len(parts) else parts[i] for i in range(0, len(parts), 2)]
            return parts[0], copies

        gram, copies = gather(gram, group_a, rank_a, partner_a, gramsrc, gather_a, a_send, a_recv)
        sent += copies
        gram, copies = gather(gram, group_b, rank_b, partner_b, sumsrc, gather_b, b_send, b_recv)
        sent += copies

        size = 4 * (STEPS + 1)
        row = lax.broadcasted_iota(jnp.int32, (size, 128), 0)
        columns = []
        for n in range(size):
            pieces = []
            for block in range(STEPS + 1):
                if n < 4 * block + 4:
                    at = 16 * block + n
                    pieces.append(jnp.broadcast_to(gram[:, at : at + 1], (4, 128)))
                else:
                    pieces.append(jnp.zeros((4, 128), jnp.float32))
            columns.append(jnp.concatenate(pieces, axis=0))
        at_zero = [
            1.0,
            -SHIFT,
            SHIFT * SHIFT - BETA1,
            -SHIFT * SHIFT * SHIFT + SHIFT * (BETA1 + BETA2),
        ]
        rights = []
        for r in range(4):
            value = jnp.zeros((size, 128), jnp.float32)
            for block in range(STEPS + 1):
                value = jnp.where(row == 4 * block + r, at_zero[block], value)
            rights.append(value)
        inverses = []
        factors = []
        for k in range(size):
            column = columns[k]
            inverse = 1.0 / column[k : k + 1, :]
            factor = jnp.where(row > k, column * inverse, 0.0)
            inverses.append(inverse)
            factors.append(factor)
            for j in range(k + 1, size):
                columns[j] = columns[j] - factor * column[j : j + 1, :]
            for r in range(4):
                rights[r] = rights[r] - factor * rights[r][k : k + 1, :]
        for r in range(4):
            value = rights[r]
            scale = jnp.concatenate(inverses, axis=0)
            value = value * scale
            for k in range(size - 2, -1, -1):
                below = jnp.sum(factors[k] * value, axis=0, keepdims=True)
                value = value - jnp.where(row == k, below, 0.0)
            rights[r] = value
        small = []
        for r in range(4):
            value = at_zero[0] * rights[r][0:4]
            for block in range(1, STEPS + 1):
                value = value + at_zero[block] * rights[r][4 * block : 4 * block + 4]
            small.append(value)
        for k in range(4):
            inverse = 1.0 / small[k][k : k + 1, :]
            small[k] = small[k] * inverse
            rights[k] = rights[k] * inverse
            for r in range(4):
                if r != k:
                    scale = small[r][k : k + 1, :]
                    small[r] = small[r] - scale * small[k]
                    rights[r] = rights[r] - scale * rights[k]

        for r in range(4):
            c = [[rights[r][4 * block + q : 4 * block + q + 1, :] for q in range(4)] for block in range(4)]
            d = [[], [], []]
            for q in range(4):
                d[0].append(SHIFT * c[2][q] - c[1][q] - (SHIFT * SHIFT - BETA2) * c[3][q])
                d[1].append(SHIFT * c[3][q] - c[2][q])
                d[2].append(-c[3][q])
            residual = jnp.zeros((5, 8, 128), jnp.float32)
            answer = jnp.zeros((5, 8, 128), jnp.float32)
            for block in range(4):
                for q in range(4):
                    values = basis[block, q]
                    residual = residual + values * c[block][q][None]
                    if block < 3:
                        answer = answer + values * d[block][q][None]
            res_ref[r] = residual
            sol_ref[r] = answer

        for copy in sent:
            copy.wait_send()

    return kernel, group_a, group_b


def solution(mesh):
    nx, ny, nz = mesh.shape["gx"], mesh.shape["gy"], mesh.shape["gz"]
    kernel, group_a, group_b = make_kernel(nx, ny, nz)
    f32 = jnp.float32
    count = len(OFFSETS)

    def shards(right_side, jacobian):
        field = jax.ShapeDtypeStruct((4, 5, 8, 128), f32)
        answer, residual = pl.pallas_call(
            kernel,
            out_shape=(field, field),
            in_specs=[
                pl.BlockSpec(memory_space=pltpu.VMEM),
                pl.BlockSpec(memory_space=pl.ANY),
            ],
            out_specs=(
                pl.BlockSpec(memory_space=pltpu.VMEM),
                pl.BlockSpec(memory_space=pltpu.VMEM),
            ),
            scratch_shapes=[
                pltpu.VMEM((675, 8, 128), jnp.bfloat16),
                pltpu.VMEM((675, 8, 128), f32),
                pltpu.VMEM((STEPS + 1, 4, 5, 8, 128), f32),
                pltpu.VMEM((STEPS, 2, 4, 5, 8, 128), f32),
                pltpu.VMEM((STEPS, 3, 2, 24, 128), f32),
                pltpu.VMEM((STEPS, 3, 2, 8, 128), f32),
                pltpu.VMEM((STEPS, 3, 4, 1, 128), f32),
                pltpu.VMEM((STEPS, 2, 24, 128), f32),
                pltpu.VMEM((STEPS, 2, 8, 128), f32),
                pltpu.VMEM((STEPS, 4, 1, 128), f32),
                pltpu.VMEM((3, 3, 4, 5, 24, 128), f32),
                pltpu.VMEM((4, 128), f32),
                pltpu.VMEM((4, 128), f32),
                pltpu.VMEM((group_a, 4, 128), f32),
                pltpu.VMEM((group_b, 4, 128), f32),
                pltpu.SemaphoreType.DMA,
                pltpu.SemaphoreType.DMA((STEPS, count)),
                pltpu.SemaphoreType.DMA((STEPS, count)),
                pltpu.SemaphoreType.DMA((group_a,)),
                pltpu.SemaphoreType.DMA((group_a,)),
                pltpu.SemaphoreType.DMA((group_b,)),
                pltpu.SemaphoreType.DMA((group_b,)),
            ],
            compiler_params=pltpu.CompilerParams(
                collective_id=0, has_side_effects=True, vmem_limit_bytes=40 * 1024 * 1024
            ),
        )(right_side.reshape(4, 5, 8, 128), jacobian.reshape(675, 8, 128))
        return answer.reshape(right_side.shape), residual.reshape(right_side.shape)

    return jax.shard_map(
        shards,
        mesh=mesh,
        in_specs=(P(None, None, "gx", "gy", "gz"), P(None, None, None, "gx", "gy", "gz")),
        out_specs=(P(None, None, "gx", "gy", "gz"), P(None, None, "gx", "gy", "gz")),
        check_vma=False,
    )
```

```python
import jax
import jax.numpy as jnp
from jax import lax
from jax.experimental import pallas as pl
from jax.experimental.pallas import tpu as pltpu
from jax.sharding import PartitionSpec as P

MESH = pl.DeviceIdType.MESH
SHIFT = 9.0
BETA1 = 3.9
BETA2 = 3.2
STEPS = 3
ROW = 8

OFFSETS = [
    (ex, ey, ez)
    for ey, ez in ((-1, -1), (-1, 1), (1, -1), (1, 1), (0, -1), (0, 1), (-1, 0), (1, 0), (0, 0))
    for ex in (-1, 1, 0)
    if (ex, ey, ez) != (0, 0, 0)
]


def side(sign):
    return (sign + 1) // 2


def make_kernel(nx, ny, nz):
    group_a = (nx // 4) * ny
    group_b = 4 * nz

    def kernel(
        rhs_hbm, jac_hbm, sol_ref, res_ref,
        jac_raw, jac, basis, slab, rowbuf, colbuf, corbuf, rowsrc, colsrc, corsrc, padded,
        gramsrc, sumsrc, gather_a, gather_b,
        rhs_sem, jac_sem, halo_send, halo_recv, a_send, a_recv, b_send, b_recv,
    ):
        ix, iy, iz = lax.axis_index("gx"), lax.axis_index("gy"), lax.axis_index("gz")

        def neighbour(offset):
            ex, ey, ez = offset
            return (
                lax.rem(ix + ex + nx, nx),
                lax.rem(iy + ey + ny, ny),
                lax.rem(iz + ez + nz, nz),
            )

        rank_a = (ix // 4) * ny + iy
        rank_b = lax.rem(ix, 4) * nz + iz

        def partner_a(offset):
            rank = lax.rem(rank_a + offset, group_a)
            return ((rank // ny) * 4 + lax.rem(ix, 4), lax.rem(rank, ny), iz)

        def partner_b(offset):
            rank = lax.rem(rank_b + offset, group_b)
            return ((ix // 4) * 4 + rank // nz, iy, lax.rem(rank, nz))

        rhs_copy = pltpu.make_async_copy(rhs_hbm, basis.at[0], rhs_sem)
        rhs_copy.start()
        jac_copy = pltpu.make_async_copy(jac_hbm, jac_raw, jac_sem)
        jac_copy.start()

        barrier = pltpu.get_barrier_semaphore()
        partners = [neighbour(offset) for offset in OFFSETS]
        partners += [partner_a(offset) for offset in range(1, group_a)]
        partners += [partner_b(offset) for offset in range(1, group_b)]
        for partner in partners:
            pl.semaphore_signal(barrier, inc=1, device_id=partner, device_id_type=MESH)

        lane = lax.broadcasted_iota(jnp.int32, (8, 128), 1)
        lane3 = lax.broadcasted_iota(jnp.int32, (4, 8, 128), 2)
        at_low = iz == 0
        at_high = iz == nz - 1

        def halo_copies(step):
            copies = []
            for index, offset in enumerate(OFFSETS):
                ex, ey, ez = offset
                if ey == 0 and ez == 0:
                    src, dst = basis.at[step], slab.at[step, side(-ex)]
                elif ez == 0:
                    src, dst = rowsrc.at[step, side(ey)], rowbuf.at[step, 1 - ex, side(-ey)]
                elif ey == 0:
                    src, dst = colsrc.at[step, side(ez)], colbuf.at[step, 1 - ex, side(-ez)]
                else:
                    src = corsrc.at[step, 2 * side(ey) + side(ez)]
                    dst = corbuf.at[step, 1 - ex, 2 * side(-ey) + side(-ez)]
                copies.append(
                    pltpu.make_async_remote_copy(
                        src_ref=src,
                        dst_ref=dst,
                        send_sem=halo_send.at[step, index],
                        recv_sem=halo_recv.at[step, index],
                        device_id=neighbour(offset),
                        device_id_type=MESH,
                    )
                )
            return copies

        def pack(step):
            low = jnp.zeros((8, 128), jnp.float32)
            high = jnp.zeros((8, 128), jnp.float32)
            for r in range(4):
                for b in range(5):
                    field = 5 * r + b
                    tile = basis[step, r, b]
                    low = jnp.where(lane == field, pltpu.roll(tile, field, 1) if field else tile, low)
                    high = jnp.where(lane == field, pltpu.roll(tile, field + 1, 1), high)
                    rowsrc[step, 0, field : field + 1, :] = tile[0:1, :]
                    rowsrc[step, 1, field : field + 1, :] = tile[7:8, :]
            colsrc[step, 0] = low
            colsrc[step, 1] = high
            for pos in range(2):
                edge = slice(7 * pos, 7 * pos + 1)
                corsrc[step, 2 * pos] = low[edge, :]
                corsrc[step, 2 * pos + 1] = high[edge, :]

        row_id = lax.broadcasted_iota(jnp.int32, (24, 128), 0)
        lane_row = lax.broadcasted_iota(jnp.int32, (24, 128), 1)

        def fill(step, plane, source):
            for dz in (-1, 0, 1):
                if dz != 0:
                    column = colbuf[step, plane, side(dz)]
                    outside = at_low if dz < 0 else at_high
                    column = jnp.where(outside, jnp.zeros_like(column), column)
                    edge_lane = 0 if dz < 0 else 127
                    turn = 1 if dz < 0 else 127
                for r in range(4):
                    for b in range(5):
                        tile = source[r, b]
                        if dz != 0:
                            field = 5 * r + b
                            shift = (edge_lane - field) % 128
                            moved = pltpu.roll(column, shift, 1) if shift else column
                            tile = jnp.where(lane == edge_lane, moved, pltpu.roll(tile, turn, 1))
                        padded[plane, dz + 1, r, b, ROW : ROW + 8, :] = tile
                for dy in (-1, 1):
                    rows = rowbuf[step, plane, side(dy)]
                    if dz != 0:
                        corner = corbuf[step, plane, 2 * side(dy) + side(dz)]
                        spread = jnp.broadcast_to(corner, (24, 128))
                        spread = jnp.where(row_id == lane_row, spread, 0.0)
                        corner_column = jnp.sum(spread, axis=1, keepdims=True)
                        corner_column = jnp.where(outside, jnp.zeros_like(corner_column), corner_column)
                        rows = jnp.where(lane_row == edge_lane, corner_column, pltpu.roll(rows, turn, 1))
                    target = ROW - 1 if dy < 0 else ROW + 8
                    for r in range(4):
                        for b in range(5):
                            field = 5 * r + b
                            padded[plane, dz + 1, r, b, target : target + 1, :] = rows[field : field + 1, :]

        def accumulate(plane, totals):
            def at_dz(dzi, totals):
                totals = list(totals)
                for dyi in range(3):
                    start = ROW - 1 + dyi
                    s = plane * 9 + dyi * 3 + dzi
                    for b in range(5):
                        values = padded[plane, dzi, :, b, start : start + 8, :]
                        for a in range(5):
                            totals[a] = totals[a] + jac[s * 25 + 5 * a + b][None] * values
                return tuple(totals)

            return lax.fori_loop(0, 3, at_dz, totals)

        def gram_block(block):
            gram = jnp.zeros((4, 128), jnp.float32)
            lanes = lax.broadcasted_iota(jnp.int32, (4, 128), 1)
            for n in range(4 * block + 4):
                product = basis[block, :, 0] * basis[n // 4, n % 4, 0][None]
                for b in range(1, 5):
                    product = product + basis[block, :, b] * basis[n // 4, n % 4, b][None]
                partial = jnp.sum(jnp.sum(product, axis=1), axis=1, keepdims=True)
                gram = jnp.where(lanes == 16 * block + n, partial, gram)
            return gram

        rhs_copy.wait()
        pack(0)
        jac_copy.wait()

        def unpack(s, carry):
            rows = pl.ds(s * 25, 25)
            jac[rows] = jac_raw[rows].astype(jnp.float32)
            return carry

        lax.fori_loop(0, 27, unpack, 0)
        for a in range(5):
            jac[13 * 25 + 6 * a] = jac[13 * 25 + 6 * a] - SHIFT

        pl.semaphore_wait(barrier, len(partners))

        sent = []
        gram = jnp.zeros((4, 128), jnp.float32)
        for step in range(STEPS):
            copies = halo_copies(step)
            for copy in copies:
                copy.start()
            sent += copies
            gram = gram + gram_block(step)
            totals = tuple(jnp.zeros((4, 8, 128), jnp.float32) for _ in range(5))
            for plane in (1, 0, 2):
                for copy, offset in zip(copies, OFFSETS):
                    if 1 - offset[0] == plane:
                        copy.wait_recv()
                fill(step, plane, basis.at[step] if plane == 1 else slab.at[step, plane // 2])
                totals = accumulate(plane, totals)
            for a in range(5):
                value = totals[a]
                if step == 1:
                    value = value - BETA1 * basis[0, :, a]
                if step == 2:
                    value = value - BETA2 * basis[1, :, a]
                basis[step + 1, :, a] = value
            if step + 1 < STEPS:
                pack(step + 1)
        gram = gram + gram_block(3)

        def gather(partial, size, rank, partner, src, slots, send, recv):
            src[...] = partial
            slots[rank] = partial
            copies = []
            for offset in range(1, size):
                copies.append(
                    pltpu.make_async_remote_copy(
                        src_ref=src,
                        dst_ref=slots.at[rank],
                        send_sem=send.at[offset],
                        recv_sem=recv.at[offset],
                        device_id=partner(offset),
                        device_id_type=MESH,
                    )
                )
            for copy in copies:
                copy.start()
            for copy in copies:
                copy.wait_recv()
            parts = [slots[i] for i in range(size)]
            while len(parts) > 1:
                parts = [parts[i] + parts[i + 1] if i + 1 < len(parts) else parts[i] for i in range(0, len(parts), 2)]
            return parts[0], copies

        gram, copies = gather(gram, group_a, rank_a, partner_a, gramsrc, gather_a, a_send, a_recv)
        sent += copies
        gram, copies = gather(gram, group_b, rank_b, partner_b, sumsrc, gather_b, b_send, b_recv)
        sent += copies

        size = 4 * (STEPS + 1)
        row = lax.broadcasted_iota(jnp.int32, (size, 128), 0)
        columns = []
        for n in range(size):
            pieces = []
            for block in range(STEPS + 1):
                if n < 4 * block + 4:
                    at = 16 * block + n
                    pieces.append(jnp.broadcast_to(gram[:, at : at + 1], (4, 128)))
                else:
                    pieces.append(jnp.zeros((4, 128), jnp.float32))
            columns.append(jnp.concatenate(pieces, axis=0))
        at_zero = [
            1.0,
            -SHIFT,
            SHIFT * SHIFT - BETA1,
            -SHIFT * SHIFT * SHIFT + SHIFT * (BETA1 + BETA2),
        ]
        rights = []
        for r in range(4):
            value = jnp.zeros((size, 128), jnp.float32)
            for block in range(STEPS + 1):
                value = jnp.where(row == 4 * block + r, at_zero[block], value)
            rights.append(value)
        inverses = []
        factors = []
        for k in range(size):
            column = columns[k]
            inverse = 1.0 / column[k : k + 1, :]
            factor = jnp.where(row > k, column * inverse, 0.0)
            inverses.append(inverse)
            factors.append(factor)
            for j in range(k + 1, size):
                columns[j] = columns[j] - factor * column[j : j + 1, :]
            for r in range(4):
                rights[r] = rights[r] - factor * rights[r][k : k + 1, :]
        for r in range(4):
            value = rights[r]
            scale = jnp.concatenate(inverses, axis=0)
            value = value * scale
            for k in range(size - 2, -1, -1):
                below = jnp.sum(factors[k] * value, axis=0, keepdims=True)
                value = value - jnp.where(row == k, below, 0.0)
            rights[r] = value
        small = []
        for r in range(4):
            value = at_zero[0] * rights[r][0:4]
            for block in range(1, STEPS + 1):
                value = value + at_zero[block] * rights[r][4 * block : 4 * block + 4]
            small.append(value)
        for k in range(4):
            inverse = 1.0 / small[k][k : k + 1, :]
            small[k] = small[k] * inverse
            rights[k] = rights[k] * inverse
            for r in range(4):
                if r != k:
                    scale = small[r][k : k + 1, :]
                    small[r] = small[r] - scale * small[k]
                    rights[r] = rights[r] - scale * rights[k]

        for r in range(4):
            c = [[rights[r][4 * block + q : 4 * block + q + 1, :] for q in range(4)] for block in range(4)]
            d = [[], [], []]
            for q in range(4):
                d[0].append(SHIFT * c[2][q] - c[1][q] - (SHIFT * SHIFT - BETA2) * c[3][q])
                d[1].append(SHIFT * c[3][q] - c[2][q])
                d[2].append(-c[3][q])
            residual = jnp.zeros((5, 8, 128), jnp.float32)
            answer = jnp.zeros((5, 8, 128), jnp.float32)
            for block in range(4):
                for q in range(4):
                    values = basis[block, q]
                    residual = residual + values * c[block][q][None]
                    if block < 3:
                        answer = answer + values * d[block][q][None]
            res_ref[r] = residual
            sol_ref[r] = answer

        for copy in sent:
            copy.wait_send()

    return kernel, group_a, group_b


def solution(mesh):
    nx, ny, nz = mesh.shape["gx"], mesh.shape["gy"], mesh.shape["gz"]
    kernel, group_a, group_b = make_kernel(nx, ny, nz)
    f32 = jnp.float32
    count = len(OFFSETS)

    def shards(right_side, jacobian):
        field = jax.ShapeDtypeStruct((4, 5, 8, 128), f32)
        answer, residual = pl.pallas_call(
            kernel,
            out_shape=(field, field),
            in_specs=[
                pl.BlockSpec(memory_space=pltpu.HBM),
                pl.BlockSpec(memory_space=pltpu.HBM),
            ],
            out_specs=(
                pl.BlockSpec(memory_space=pltpu.VMEM),
                pl.BlockSpec(memory_space=pltpu.VMEM),
            ),
            scratch_shapes=[
                pltpu.VMEM((675, 8, 128), jnp.bfloat16),
                pltpu.VMEM((675, 8, 128), f32),
                pltpu.VMEM((STEPS + 1, 4, 5, 8, 128), f32),
                pltpu.VMEM((STEPS, 2, 4, 5, 8, 128), f32),
                pltpu.VMEM((STEPS, 3, 2, 24, 128), f32),
                pltpu.VMEM((STEPS, 3, 2, 8, 128), f32),
                pltpu.VMEM((STEPS, 3, 4, 1, 128), f32),
                pltpu.VMEM((STEPS, 2, 24, 128), f32),
                pltpu.VMEM((STEPS, 2, 8, 128), f32),
                pltpu.VMEM((STEPS, 4, 1, 128), f32),
                pltpu.VMEM((3, 3, 4, 5, 24, 128), f32),
                pltpu.VMEM((4, 128), f32),
                pltpu.VMEM((4, 128), f32),
                pltpu.VMEM((group_a, 4, 128), f32),
                pltpu.VMEM((group_b, 4, 128), f32),
                pltpu.SemaphoreType.DMA,
                pltpu.SemaphoreType.DMA,
                pltpu.SemaphoreType.DMA((STEPS, count)),
                pltpu.SemaphoreType.DMA((STEPS, count)),
                pltpu.SemaphoreType.DMA((group_a,)),
                pltpu.SemaphoreType.DMA((group_a,)),
                pltpu.SemaphoreType.DMA((group_b,)),
                pltpu.SemaphoreType.DMA((group_b,)),
            ],
            compiler_params=pltpu.CompilerParams(
                collective_id=0, has_side_effects=True, vmem_limit_bytes=56360960
            ),
        )(right_side.reshape(4, 5, 8, 128), jacobian.reshape(675, 8, 128))
        return answer.reshape(right_side.shape), residual.reshape(right_side.shape)

    return jax.shard_map(
        shards,
        mesh=mesh,
        in_specs=(P(None, None, "gx", "gy", "gz"), P(None, None, None, "gx", "gy", "gz")),
        out_specs=(P(None, None, "gx", "gy", "gz"), P(None, None, "gx", "gy", "gz")),
        check_vma=False,
    )
```
